1024 devices in a mesh: rows: 1024 (over z, y, x, core).
Axes of the slice: x: 8, y: 8, z: 8, core: 2. Of those that a mesh axis runs over, the one named last changes fastest.
Arguments:
- snapshots: float32 [524288, 512], P('rows'), may hold values from -100 to 100
- validation: float32 [524288, 512], P('rows'), may hold values from -100 to 100
- eigenvectors: float32 [512, 64], replicated, may hold values from -0.25 to 0.25
- eigenvalues: float32 [64], replicated, may hold values from 16 to 256
Outputs:
- gram: float32 [512, 512], replicated
- modes: float32 [64, 524288], P(None, 'rows')
- train_coef: float32 [64, 512], replicated
- valid_coef: float32 [64, 512], replicated
The draws below stay inside these ranges and needn't reach their ends.
All inputs are finite; a program needn't handle non-finite values.
Results may differ from the reference program's by a relative error of at most 0.000071.
Values sent between devices are 32-bit elements; how exact they have to be, the bound alone decides.
A program may use at most 32 MiB of HBM per device.

```python
import math
import jax
import jax.numpy as jnp
from jax import lax

K = 512
M = 64
NDOF = 524288


def common_parts(key):
    base = jax.random.fold_in(key, 7)
    first, second, third = jax.random.split(base, 3)
    spread = jnp.exp(jax.random.uniform(first, (NDOF, 1), jnp.float32, 0.0, 0.5 * math.log(10.0)))
    rising = jnp.sqrt(1.0 + 2.0 * jnp.arange(NDOF, dtype=jnp.float32) / NDOF)[:, None]
    columns = jnp.exp(jax.random.uniform(third, (1, K), jnp.float32, 0.0, 0.25 * math.log(10.0)))
    noise = jnp.clip(jax.random.normal(second, (NDOF, K), jnp.float32), -6.0, 6.0)
    return (spread * rising * columns, noise)


def draw_snapshots(key, part):
    scaling, noise = common_parts(key)
    return scaling * noise


def draw_validation(key, part):
    scaling, noise = common_parts(key)
    other = jax.random.fold_in(key, 11)
    fresh = jnp.clip(jax.random.normal(other, (NDOF, K), jnp.float32), -6.0, 6.0)
    return scaling * (0.8 * noise + 0.6 * fresh)


def centred(rng, extent, scale, limit, kind=jnp.bfloat16):
    entries = scale * jax.random.normal(rng, extent, jnp.float32)
    return jnp.clip(entries, min=-limit, max=limit).astype(kind)


def setup_inputs(seed: int = 0) -> dict:
    arg_keys = jax.random.split(jax.random.key(seed), 5)
    snapshots = draw_snapshots(jax.random.fold_in(arg_keys[4], 71), 0)
    validation = draw_validation(jax.random.fold_in(arg_keys[4], 71), 0)
    eigenvectors = centred(arg_keys[2], (K, M), K ** -0.5, 0.25, jnp.float32)
    eigenvalues = jnp.clip(jnp.exp(jax.random.uniform(arg_keys[3], (M,), jnp.float32, math.log(16.0), math.log(256.0))), 16.0, 256.0)
    return {"snapshots": snapshots, "validation": validation, "eigenvectors": eigenvectors, "eigenvalues": eigenvalues}


def reference(snapshots, validation, eigenvectors, eigenvalues):
    highest = lax.Precision.HIGHEST
    total = snapshots.shape[0] * 1.0
    gram = lax.dot_general(snapshots, snapshots, (((0,), (0,)), ((), ())), precision=highest, preferred_element_type=jnp.float32) / total
    scales = lax.rsqrt(eigenvalues)
    modes = lax.dot_general(eigenvectors, snapshots, (((0,), (1,)), ((), ())), precision=highest, preferred_element_type=jnp.float32) * scales[:, None]
    train_coef = jnp.dot(modes, snapshots, precision=highest, preferred_element_type=jnp.float32) / total
    valid_coef = jnp.dot(modes, validation, precision=highest, preferred_element_type=jnp.float32) / total
    return (gram, modes, train_coef, valid_coef)
```

```python
import functools

import jax
import jax.numpy as jnp
from jax import lax
from jax.experimental import pallas as pl
from jax.experimental.pallas import tpu as pltpu
from jax.sharding import PartitionSpec as P

MESH = pl.DeviceIdType.MESH
F32 = jnp.float32
BF16 = jnp.bfloat16
UNIT = 256
BLOCKS = [(0, 0), (0, 1), (1, 1), (0, 2), (0, 3), (1, 2), (1, 3), (2, 2), (2, 3), (3, 3)]


def split(x):
    hi = x.astype(BF16)
    return hi, (x - hi.astype(F32)).astype(BF16)


def dot(a, b):
    return jnp.dot(a, b, preferred_element_type=F32)


def dot_nt(a, b):
    return lax.dot_general(a, b, (((1,), (1,)), ((), ())), preferred_element_type=F32)


def three(f, a, b):
    (ah, al), (bh, bl) = a, b
    return f(ah, bh) + (f(ah, bl) + f(al, bh))


def scaled_vectors(vec_ref, val_ref):
    return jnp.transpose(vec_ref[...] * lax.rsqrt(val_ref[...]))


def reduce_kernel(
    side, inv_total, snap_hbm, valid_hbm, vec_ref, val_ref, full_ref, modes_ref,
    snap, valid, xh, xl, xht, xlt, pay, pair, acc, ring1, mine, ring2, ring3,
    in_sem, pair_send, pair_recv, send_sem, recv_sem, last_send, last_recv,
):
    me = lax.axis_index("rows")
    core = lax.rem(me, 2)
    strides = (2, 2 * side, 2 * side * side)
    spots = [lax.rem(me // s, side) for s in strides]
    partner = me + 1 - 2 * core
    piece = UNIT // side

    def peer(axis, d):
        return me + (lax.rem(spots[axis] + d, side) - spots[axis]) * strides[axis]

    def each(f):
        def step(d, carry):
            f(d)
            return carry

        lax.fori_loop(1, side, step, 0)

    barrier = pltpu.get_barrier_semaphore()
    for axis in range(3):
        each(
            lambda d, axis=axis: pl.semaphore_signal(
                barrier, inc=1, device_id=(peer(axis, d),), device_id_type=MESH
            )
        )
    pl.semaphore_signal(barrier, inc=1, device_id=(partner,), device_id_type=MESH)

    load_snap = pltpu.make_async_copy(snap_hbm, snap, in_sem.at[0])
    load_valid = pltpu.make_async_copy(valid_hbm, valid, in_sem.at[1])
    load_snap.start()
    load_valid.start()
    load_snap.wait()

    h, l = split(snap[...])
    xh[...] = h
    xl[...] = l
    xht[...] = jnp.transpose(h)
    xlt[...] = jnp.transpose(l)
    for big, (p, q) in enumerate([(0, 0), (0, 1), (1, 1)]):
        rows, cols = pl.ds(p * 256, 256), pl.ds(q * 256, 256)
        g = three(dot, (xht[rows, :], xlt[rows, :]), (xh[:, cols], xl[:, cols])) * inv_total
        for k, (i, j) in enumerate(BLOCKS):
            if (i // 2, j // 2) == (p, q):
                r, c = 128 * (i % 2), 128 * (j % 2)
                pay[k // 2, pl.ds(128 * (k % 2), 128), :] = g[r : r + 128, c : c + 128]
    vectors = split(scaled_vectors(vec_ref, val_ref))
    modes = three(dot_nt, vectors, (xh[...], xl[...]))
    modes_ref[...] = modes
    load_valid.wait()
    part = three(dot, split(modes), split(valid[...])) * inv_total
    for j in range(4):
        pay[5, pl.ds(64 * j, 64), :] = part[:, 128 * j : 128 * j + 128]

    pl.semaphore_wait(barrier, 3 * (side - 1) + 1)

    pairs = []
    for t in range(3):
        c = pltpu.make_async_remote_copy(
            src_ref=pay.at[2 * t + 1 - core], dst_ref=pair.at[t],
            send_sem=pair_send.at[t], recv_sem=pair_recv.at[t],
            device_id=(partner,), device_id_type=MESH,
        )
        c.start()
        pairs.append(c)

    def rows_of(k):
        return pl.ds(pl.multiple_of(k * piece, piece), piece)

    def copy(stage, t, d):
        axis = (t + (0, 1, 2, 0)[stage]) % 3
        spot = spots[axis]
        if stage == 0:
            src = acc.at[t, rows_of(lax.rem(spot + d, side)), :]
            dst = ring1.at[t, d - 1]
        elif stage == 1:
            src, dst = mine.at[t], ring2.at[t, spot]
        elif stage == 2:
            src, dst = mine.at[3 + t], ring3.at[t, spot]
        else:
            src = mine.at[6 + t]
            dst = full_ref.at[2 * t + core, rows_of(spot), :]
        k = (stage * 3 + t) * side + d
        return pltpu.make_async_remote_copy(
            src_ref=src, dst_ref=dst, send_sem=send_sem.at[k], recv_sem=recv_sem.at[k],
            device_id=(peer(axis, d),), device_id_type=MESH,
        )

    for t in range(3):
        pairs[t].wait_recv()
        acc[t] = pay[2 * t + core] + pair[t]
        each(lambda d, t=t: copy(0, t, d).start())
    for t in range(3):
        each(lambda d, t=t: copy(0, t, d).wait_recv())
        total = acc[t, rows_of(spots[t]), :]
        for d in range(side - 1):
            total += ring1[t, d]
        mine[t] = total
        ring2[t, spots[(t + 1) % 3]] = total
        each(lambda d, t=t: copy(1, t, d).start())
    for t in range(3):
        each(lambda d, t=t: copy(1, t, d).wait_recv())
        total = ring2[t, 0]
        for d in range(1, side):
            total += ring2[t, d]
        mine[3 + t] = total
        ring3[t, spots[(t + 2) % 3]] = total
        each(lambda d, t=t: copy(2, t, d).start())
    for t in range(3):
        each(lambda d, t=t: copy(2, t, d).wait_recv())
        total = ring3[t, 0]
        for d in range(1, side):
            total += ring3[t, d]
        mine[6 + t] = total
        full_ref[2 * t + core, rows_of(spots[t]), :] = total
        each(lambda d, t=t: copy(3, t, d).start())

    def last(t, d):
        spot = lax.rem(spots[t] + side - d, side)
        ref = full_ref.at[2 * t + core, rows_of(spot), :]
        src = mine.at[6 + t] if isinstance(d, int) and d == 0 else ref
        k = t * side + d
        return pltpu.make_async_remote_copy(
            src_ref=src, dst_ref=ref, send_sem=last_send.at[k], recv_sem=last_recv.at[k],
            device_id=(partner,), device_id_type=MESH,
        )

    for t in range(3):
        last(t, 0).start()
    for t in range(3):

        def forward(d, t=t):
            copy(3, t, d).wait_recv()
            last(t, d).start()

        each(forward)
    for stage in range(4):
        for t in range(3):
            each(lambda d, stage=stage, t=t: copy(stage, t, d).wait_send())
    for t in range(3):
        pairs[t].wait_send()

        def end(d, carry, t=t):
            spot = lax.rem(spots[t] + side - d, side)
            arrived = full_ref.at[2 * t + 1 - core, rows_of(spot), :]
            k = t * side + d
            c = pltpu.make_async_remote_copy(
                src_ref=arrived, dst_ref=arrived, send_sem=last_send.at[k],
                recv_sem=last_recv.at[k], device_id=(partner,), device_id_type=MESH,
            )
            c.wait_send()
            c.wait_recv()
            return carry

        lax.fori_loop(0, side, end, 0)


def finish_kernel(full_ref, vec_ref, val_ref, modes_in, gram_ref, modes_ref, train_ref, valid_ref):
    for k, (i, j) in enumerate(BLOCKS):
        b = full_ref[k // 2, pl.ds(128 * (k % 2), 128), :]
        gram_ref[pl.ds(128 * i, 128), pl.ds(128 * j, 128)] = b
        if i != j:
            gram_ref[pl.ds(128 * j, 128), pl.ds(128 * i, 128)] = jnp.transpose(b)
    for j in range(4):
        valid_ref[:, pl.ds(128 * j, 128)] = full_ref[5, pl.ds(64 * j, 64), :]
    modes_ref[...] = modes_in[...]
    train_ref[...] = three(dot, split(scaled_vectors(vec_ref, val_ref)), split(gram_ref[...]))


def body(snapshots, validation, eigenvectors, eigenvalues, *, side):
    rows, count = snapshots.shape
    modes = eigenvectors.shape[1]
    devices = 2 * side**3
    piece = UNIT // side
    values = eigenvalues.reshape(1, modes)
    vmem = pl.BlockSpec(memory_space=pltpu.VMEM)
    hbm = pl.BlockSpec(memory_space=pl.ANY)
    dma = pltpu.SemaphoreType.DMA
    full, modes_part = pl.pallas_call(
        functools.partial(reduce_kernel, side, 1.0 / (rows * devices)),
        out_shape=(
            jax.ShapeDtypeStruct((6, UNIT, 128), F32),
            jax.ShapeDtypeStruct((modes, rows), F32),
        ),
        in_specs=[hbm, hbm, vmem, vmem],
        out_specs=(vmem, vmem),
        scratch_shapes=[
            pltpu.VMEM((rows, count), F32),
            pltpu.VMEM((rows, count), F32),
            pltpu.VMEM((rows, count), BF16),
            pltpu.VMEM((rows, count), BF16),
            pltpu.VMEM((count, rows), BF16),
            pltpu.VMEM((count, rows), BF16),
            pltpu.VMEM((6, UNIT, 128), F32),
            pltpu.VMEM((3, UNIT, 128), F32),
            pltpu.VMEM((3, UNIT, 128), F32),
            pltpu.VMEM((3, side - 1, piece, 128), F32),
            pltpu.VMEM((9, piece, 128), F32),
            pltpu.VMEM((3, side, piece, 128), F32),
            pltpu.VMEM((3, side, piece, 128), F32),
            dma((2,)),
            dma((3,)),
            dma((3,)),
            dma((12 * side,)),
            dma((12 * side,)),
            dma((3 * side,)),
            dma((3 * side,)),
        ],
        compiler_params=pltpu.CompilerParams(collective_id=0, has_side_effects=True),
        name="reduce",
    )(snapshots, validation, eigenvectors, values)
    return pl.pallas_call(
        finish_kernel,
        out_shape=(
            jax.ShapeDtypeStruct((count, count), F32),
            jax.ShapeDtypeStruct((modes, rows), F32),
            jax.ShapeDtypeStruct((modes, count), F32),
            jax.ShapeDtypeStruct((modes, count), F32),
        ),
        in_specs=[vmem] * 4,
        out_specs=(vmem,) * 4,
        name="finish",
    )(full, eigenvectors, values, modes_part)


def solution(mesh):
    side = round((mesh.shape["rows"] // 2) ** (1 / 3))
    in_specs = (P("rows", None), P("rows", None), P(), P())
    out_specs = (P(), P(None, "rows"), P(), P())
    return jax.shard_map(
        functools.partial(body, side=side),
        mesh=mesh,
        in_specs=in_specs,
        out_specs=out_specs,
        check_vma=False,
    )
```
